256 devices in a mesh: rep: 16 (over y, x), mp: 16 (over z, core).
Axes of the slice: x: 4, y: 4, z: 8, core: 2. Of those that a mesh axis runs over, the one named last changes fastest.
Arguments:
- acts: bfloat16 [4096, 512, 256], P('rep', 'mp'), may hold values from -40 to 40, as said below
- refresh: int32 [512], P(('mp', 'rep')), may hold values from 0 to 16, as said below
- damping: float32 [512], P(('mp', 'rep')), may hold values from 0.2 to 1
- old_inverse: bfloat16 [512, 256, 256], P(('mp', 'rep')), may hold values from -0.375 to 0.375
- grads: bfloat16 [1024, 512, 256], P('rep', 'mp'), may hold values from -6 to 6
Outputs:
- covariance: float32 [512, 256, 256], P(('mp', 'rep'))
- new_inverse: bfloat16 [512, 256, 256], P(('mp', 'rep'))
- precond: bfloat16 [1024, 512, 256], P('rep', 'mp')
The draws below stay inside these ranges and needn't reach their ends.
Inputs may be any that keep to these rules, and one draw needn't show every extreme that they name: `acts`: entries are bfloat16 values of order one with unequal feature scales. Block g * 32 + 2 * r + q (q = 0 or 1) is the q-th block of group g at replica index r. A block is refreshed only by a group through the same r. For every r, each group refreshes exactly one block through r. Of the two blocks of a group at r, at most one is refreshed by another group, and then the other one by the group itself. In every draw some groups refresh a block of another group.
All inputs are finite; a program needn't handle non-finite values. Where the reference program divides by a largest or mean magnitude, that divisor is 1e-20 or more.
Results may differ from the reference program's by a relative error of at most 0.009.
Values may be sent and summed in bfloat16 or wider, within the bound.
No kernel may reach another device: no remote copies, remote signals or barrier semaphores. Data moves between devices by JAX's collectives and lax.ppermute only.
A program may use at most 64 MiB of HBM per device.

```python
import math
import jax
import jax.numpy as jnp
from jax import lax

B = 256
OUT = 1024
ITERS = 5
BLK_DEV = 32
GROUPS = 16
TOKENS = 4096
NBLK = 512


def draw_acts(key, part):

    def one_block(block_index):
        block_key = jax.random.fold_in(jax.random.fold_in(key, 7), block_index)
        key_list = jax.random.split(block_key, 3)
        base_noise = jax.random.normal(key_list[0], (TOKENS, B), jnp.float32)
        scales = jnp.exp(jax.random.uniform(key_list[2], (B,), jnp.float32, jnp.log(0.5), jnp.log(2.0)))
        feature_order = jax.random.permutation(key_list[1], B)
        mixed = base_noise + 0.7 * jnp.take(base_noise, feature_order, axis=1)
        return (mixed * scales[None, :]).astype(jnp.bfloat16)
    blocks = lax.map(one_block, jnp.arange(NBLK, dtype=jnp.int32))
    return jnp.transpose(blocks, (1, 0, 2))


def draw_refresh(key, part):
    replicas = BLK_DEV // 2
    heavy_count = GROUPS * 3 // 8
    key_list = jax.random.split(jax.random.fold_in(key, 23), 2)
    row_keys = jax.random.split(key_list[0], replicas)
    arranged = jax.vmap(lambda row_key: jax.random.permutation(row_key, GROUPS))(row_keys).astype(jnp.int32)
    position = jnp.argsort(arranged, axis=1, stable=True).astype(jnp.int32)
    local_pick = jax.random.randint(key_list[1], (replicas, GROUPS), 0, 2)
    partner = jnp.take_along_axis(arranged, jnp.minimum(position + heavy_count, GROUPS - 1), axis=1)
    own_group = jnp.broadcast_to(jnp.arange(GROUPS, dtype=jnp.int32)[None, :], (replicas, GROUPS))
    is_giver = position < heavy_count
    is_taker = (position >= heavy_count) & (position < 2 * heavy_count)
    other_value = jnp.where(is_giver, partner, GROUPS)
    first_value = jnp.where(local_pick == 0, own_group, other_value)
    second_value = jnp.where(local_pick == 1, own_group, other_value)
    first_value = jnp.where(is_taker, GROUPS, first_value)
    second_value = jnp.where(is_taker, GROUPS, second_value)
    stacked = jnp.stack([first_value, second_value], axis=-1)
    return jnp.transpose(stacked, (1, 0, 2)).reshape(NBLK).astype(jnp.int32)


def levels(rng, shape, cuts, least, top_value):
    gain = 1.0
    for dim, shards_of in cuts:
        heights = jax.random.uniform(jax.random.fold_in(jax.random.fold_in(rng, 6), dim), (shards_of,), jnp.float32, least / len(cuts), top_value / len(cuts))
        gain = gain * jnp.repeat(jnp.exp(heights), shape[dim] // shards_of).reshape((-1,) + (1,) * (len(shape) - 1 - dim))
    return gain


def scatter_about(stream_key, shape, width, most, cuts=(), kind=jnp.bfloat16):
    factor_of = levels(stream_key, shape, cuts, -0.22, 0.18) if cuts else 1.0
    values = jax.random.normal(stream_key, shape, jnp.float32) * width * factor_of
    return jnp.minimum(jnp.maximum(values, -most), most).astype(kind)


def setup_inputs(seed: int = 0) -> dict:
    arg_keys = jax.random.split(jax.random.key(seed), 6)
    return {
        "acts": draw_acts(jax.random.fold_in(arg_keys[5], 71), 0),
        "refresh": draw_refresh(jax.random.fold_in(arg_keys[5], 71), 0),
        "damping": jnp.clip(jnp.exp(math.log(1.0) - 1.609438 * jax.random.uniform(arg_keys[2], (NBLK,), jnp.float32) ** levels(arg_keys[2], (NBLK,), ((0, 256),), -0.2, 0.2)), 0.2, 1.0),
        "old_inverse": scatter_about(arg_keys[3], (NBLK, B, B), B ** -0.5, 0.375, ((0, 256),)),
        "grads": scatter_about(arg_keys[4], (OUT, NBLK, B), 1.0, 6.0, ((0, 16), (1, 16))),
    }


HIGHEST_PRECISION = lax.Precision.HIGHEST


def newton_inverse(gram, damp_value):
    order_size = gram.shape[-1]
    identity = jnp.eye(order_size, dtype=jnp.float32)
    matrix = gram + damp_value * identity
    row_bound = jnp.max(jnp.sum(jnp.abs(matrix), axis=1))
    approx = identity / row_bound
    for iteration in range(ITERS):
        product = jnp.dot(matrix, approx, precision=HIGHEST_PRECISION, preferred_element_type=jnp.float32)
        approx = jnp.dot(approx, 2.0 * identity - product, precision=HIGHEST_PRECISION, preferred_element_type=jnp.float32)
    return approx


def reference(acts, refresh, damping, old_inverse, grads):
    def block_gram(block_index):
        block_acts = lax.dynamic_index_in_dim(acts, block_index, 1, keepdims=False)
        return jnp.dot(block_acts.T, block_acts, preferred_element_type=jnp.float32) / TOKENS

    covariance = lax.map(block_gram, jnp.arange(NBLK, dtype=jnp.int32))

    def invert_one(inputs_pair):
        return newton_inverse(inputs_pair[0], inputs_pair[1]).astype(jnp.bfloat16)

    refreshed = lax.map(invert_one, (covariance, damping))
    due_mask = refresh != GROUPS
    new_inverse = jnp.where(due_mask[:, None, None], refreshed, old_inverse)

    def precondition(block_index):
        grad_block = lax.dynamic_index_in_dim(grads, block_index, 1, keepdims=False)
        inverse = lax.dynamic_index_in_dim(new_inverse, block_index, 0, keepdims=False)
        return jnp.dot(grad_block, inverse, preferred_element_type=jnp.float32).astype(jnp.bfloat16)

    precond = lax.map(precondition, jnp.arange(NBLK, dtype=jnp.int32))
    return covariance, new_inverse, jnp.transpose(precond, (1, 0, 2))
```

```python
import jax
import jax.numpy as jnp
from jax import lax
from jax.experimental import pallas as pl
from jax.experimental.pallas import tpu as pltpu
from jax.sharding import PartitionSpec as P

ITERS = 5
SIDE = 4
F32 = jnp.float32
BF16 = jnp.bfloat16
VM = pl.BlockSpec(memory_space=pltpu.VMEM)
SM = pl.BlockSpec(memory_space=pltpu.SMEM)


def square_index(n):
    return (
        lax.broadcasted_iota(jnp.int32, (n, n), 0),
        lax.broadcasted_iota(jnp.int32, (n, n), 1),
    )


def lay_out(scr, value):
    for j in range(scr.shape[0]):
        scr[j] = value[:, j * 128 : (j + 1) * 128].astype(F32)


def every(scr, start, count, stride):
    planes = [scr[j, pl.ds(start, count, stride=stride), :] for j in range(scr.shape[0])]
    return jnp.concatenate(planes, axis=1).astype(BF16)


def planes_of(rows, width):
    return pltpu.VMEM((width // 128, rows, 128), F32)


def spread_rows(grads):
    rows, blocks, width = grads.shape
    chunk = 8

    def kernel(g_ref, o_ref, scr):
        for i in range(blocks // chunk):
            lay_out(scr.at[i], g_ref[:, chunk * i : chunk * (i + 1), :].reshape(rows * chunk, width))
            for k in range(chunk):
                where = (chunk * i + k) // 2
                o_ref[where, pl.ds((k % 2) * rows, rows), :] = every(scr.at[i], k, rows, chunk)

    return pl.pallas_call(
        kernel,
        out_shape=jax.ShapeDtypeStruct((blocks // 2, 2 * rows, width), BF16),
        in_specs=[VM],
        out_specs=VM,
        scratch_shapes=[pltpu.VMEM((blocks // chunk, width // 128, rows * chunk, 128), F32)],
        name="spread_rows",
    )(grads)


def merge_rows(received):
    count, twice, width = received.shape
    rows = twice // 2
    blocks = 2 * count
    chunk = 8

    def kernel(r_ref, o_ref, scr):
        for i in range(blocks // chunk):
            for k in range(chunk):
                where = (chunk * i + k) // 2
                value = r_ref[where, pl.ds((k % 2) * rows, rows), :].astype(F32)
                for j in range(width // 128):
                    scr[i, j, pl.ds(k, rows, stride=chunk), :] = value[:, j * 128 : (j + 1) * 128]
            merged = jnp.concatenate([scr[i, j] for j in range(width // 128)], axis=1)
            o_ref[:, chunk * i : chunk * (i + 1), :] = merged.astype(BF16).reshape(rows, chunk, width)

    return pl.pallas_call(
        kernel,
        out_shape=jax.ShapeDtypeStruct((rows, blocks, width), BF16),
        in_specs=[VM],
        out_specs=VM,
        scratch_shapes=[pltpu.VMEM((blocks // chunk, width // 128, rows * chunk, 128), F32)],
        name="merge_rows",
    )(received)


def place():
    rep = lax.axis_index("rep")
    return rep // SIDE, rep % SIDE, lax.axis_index("mp") % 2


def step_along(value, shift, first):
    pairs = []
    groups = lax.axis_size("mp")
    for y in range(SIDE):
        for x in range(SIDE):
            for g in range(groups):
                along_x = (g % 2 == 0) == first
                ty, tx = (y, (x + shift) % SIDE) if along_x else ((y + shift) % SIDE, x)
                pairs.append(((SIDE * y + x) * groups + g, (SIDE * ty + tx) * groups + g))
    return lax.ppermute(value, ("rep", "mp"), pairs)


def partial_grams(acts):
    tokens, blocks, width = acts.shape
    half = width // 2
    chunk = 2 * SIDE

    def kernel(a_hbm, o0_ref, o1_ref, o2_ref, o3_ref, stage, scr, sems):
        outs = (o0_ref, o1_ref, o2_ref, o3_ref)
        y, x, other = place()
        copies = [
            pltpu.make_async_copy(a_hbm.at[:, pl.ds(chunk * i, chunk), :], stage.at[i], sems.at[i])
            for i in range(SIDE)
        ]
        for copy in copies:
            copy.start()
        row, col = square_index(half)
        top_row = lax.broadcasted_iota(jnp.int32, (8, half), 0)
        for i in range(SIDE):
            copies[i].wait()
            lay_out(scr.at[i], stage[i].reshape(tokens * chunk, width))

        def body(m, carry):
            for k in range(SIDE):
                ty = lax.rem(y + jnp.where(other == 0, m, k), SIDE)
                tx = lax.rem(x + jnp.where(other == 0, k, m), SIDE)
                last = jnp.zeros((8, half), F32)
                for q in range(2):
                    v = every(scr.at[ty], 2 * tx + q, tokens, chunk)
                    gram = lax.dot_general(v, v, (((0,), (0,)), ((), ())), preferred_element_type=F32)
                    low = gram[half:, half:]
                    tri = jnp.where(row >= col, gram[:half, :half], low)
                    outs[k][m, q * width : q * width + half] = tri.astype(BF16)
                    outs[k][m, q * width + half : (q + 1) * width] = gram[:half, half:].astype(BF16)
                    diagonal = jnp.sum(jnp.where(row == col, low, 0.0), axis=0, keepdims=True)
                    last = jnp.where(top_row == q, diagonal, last)
                outs[k][m, 2 * width :] = last.astype(BF16)
            return carry

        lax.fori_loop(0, SIDE, body, 0)

    shape = jax.ShapeDtypeStruct((SIDE, 2 * width + 8, half), BF16)
    return pl.pallas_call(
        kernel,
        out_shape=(shape,) * SIDE,
        in_specs=[pl.BlockSpec(memory_space=pl.ANY)],
        out_specs=(VM,) * SIDE,
        scratch_shapes=[
            pltpu.VMEM((SIDE, tokens, chunk, width), BF16),
            pltpu.VMEM((SIDE, width // 128, tokens * chunk, 128), F32),
            pltpu.SemaphoreType.DMA((SIDE,)),
        ],
        name="partial_grams",
    )(acts)


def add_up(pieces):
    count, rows, half = pieces[0].shape

    def kernel(*refs):
        ins, outs = refs[: len(pieces)], refs[len(pieces) :]
        for m in range(count):
            total = ins[0][m].astype(F32)
            for ref in ins[1:]:
                total = total + ref[m].astype(F32)
            outs[m][...] = total.astype(outs[m].dtype)

    return pl.pallas_call(
        kernel,
        out_shape=tuple(jax.ShapeDtypeStruct((rows, half), F32 if m == 0 else BF16) for m in range(count)),
        in_specs=[VM] * len(pieces),
        out_specs=(VM,) * count,
        name="add_up",
    )(*pieces)


def split(x):
    high = x.astype(BF16)
    return high, (x - high.astype(F32)).astype(BF16)


def mul(a, b):
    return lax.dot_general(a, b, (((1,), (0,)), ((), ())), preferred_element_type=F32)


def unpack(total, q, half):
    width = 2 * half
    row, col = square_index(half)
    tri = total[q * width : q * width + half]
    tri_t = tri.T
    cross = total[q * width + half : (q + 1) * width]
    diagonal = total[2 * width + q : 2 * width + q + 1]
    top = jnp.where(row >= col, tri, tri_t)
    low = jnp.where(row < col, tri, jnp.where(row > col, tri_t, diagonal))
    return jnp.concatenate(
        [jnp.concatenate([top, cross], axis=1), jnp.concatenate([cross.T, low], axis=1)], axis=0
    )


def refresh_blocks(pieces, damping, refresh, old_inverse, rows, groups, tokens_all):
    slots, width, _ = old_inverse.shape
    half = width // 2
    count, twice, _ = rows.shape
    share = twice // slots

    def kernel(*refs):
        p_refs = refs[: len(pieces)]
        damp_ref, refresh_ref, old_ref, rows_ref, cov_ref, inv_ref, out_ref = refs[len(pieces) :]
        row, col = square_index(width)
        eye = jnp.where(row == col, 1.0, 0.0).astype(F32)
        total = p_refs[0][...].astype(F32)
        for ref in p_refs[1:]:
            total = total + ref[...].astype(F32)
        total = total * (1.0 / tokens_all)
        state = []
        for q in range(slots):
            cov = unpack(total, q, half)
            cov_ref[q] = cov
            matrix = cov + damp_ref[q] * eye
            bound = jnp.max(jnp.sum(jnp.abs(matrix), axis=0, keepdims=True), axis=1, keepdims=True)
            inv_bound = 1.0 / bound
            error = eye - matrix * inv_bound
            state.append((error, eye + error, inv_bound))
        for step in range(ITERS):
            following = []
            for error, series, inv_bound in state:
                e_high, e_low = split(error)
                if step == 0:
                    power = mul(e_high, e_high) + (mul(e_low, e_high) + mul(e_high, e_low))
                    following.append((power, series, inv_bound))
                    continue
                s_high, s_low = split(series)
                grown = mul(s_high, e_high) + (mul(s_low, e_high) + mul(s_high, e_low))
                power = error
                if step < ITERS - 1:
                    power = mul(e_high, e_high) + (mul(e_low, e_high) + mul(e_high, e_low))
                following.append((power, series + grown, inv_bound))
            state = following
        for q in range(slots):
            _, series, inv_bound = state[q]
            fresh = (series * inv_bound).astype(BF16)
            keep = (jnp.zeros((width, width), jnp.int32) + refresh_ref[q]) == groups
            inverse = jnp.where(keep, old_ref[q].astype(F32), fresh.astype(F32)).astype(BF16)
            inv_ref[q] = inverse
            flat = rows_ref[:, pl.ds(q * share, share), :].reshape(count * share, width)
            out_ref[:, pl.ds(q * share, share), :] = (
                mul(flat, inverse).astype(BF16).reshape(count, share, width)
            )

    return pl.pallas_call(
        kernel,
        out_shape=(
            jax.ShapeDtypeStruct((slots, width, width), F32),
            jax.ShapeDtypeStruct((slots, width, width), BF16),
            jax.ShapeDtypeStruct(rows.shape, BF16),
        ),
        in_specs=[VM] * len(pieces) + [SM, SM, VM, VM],
        out_specs=(VM,) * 3,
        name="refresh_blocks",
    )(*pieces, damping, refresh, old_inverse, rows)


def exchange(x):
    return lax.all_to_all(x, "rep", split_axis=0, concat_axis=0, tiled=True)


def local(acts, refresh, damping, old_inverse, grads):
    replicas = lax.axis_size("rep")
    groups = lax.axis_size("mp")
    tokens_all = acts.shape[0] * replicas
    rows = exchange(spread_rows(grads))
    pieces = partial_grams(acts)
    pieces = [pieces[0]] + [step_along(pieces[k], k, True) for k in range(1, SIDE)]
    pieces = add_up(pieces)
    pieces = [pieces[0]] + [step_along(pieces[k], k, False) for k in range(1, SIDE)]
    covariance, new_inverse, out = refresh_blocks(
        pieces, damping, refresh, old_inverse, rows, groups, tokens_all
    )
    return (covariance, new_inverse, merge_rows(exchange(out)))


def solution(mesh):
    return jax.shard_map(
        local,
        mesh=mesh,
        in_specs=(
            P("rep", "mp", None),
            P(("mp", "rep")),
            P(("mp", "rep")),
            P(("mp", "rep"), None, None),
            P("rep", "mp", None),
        ),
        out_specs=(
            P(("mp", "rep"), None, None),
            P(("mp", "rep"), None, None),
            P("rep", "mp", None),
        ),
        check_vma=False,
    )
```

```python
import jax
import jax.numpy as jnp
from jax import lax
from jax.experimental import pallas as pl
from jax.experimental.pallas import tpu as pltpu
from jax.sharding import PartitionSpec as P

ITERS = 5
SIDE = 4
F32 = jnp.float32
BF16 = jnp.bfloat16
VM = pl.BlockSpec(memory_space=pltpu.VMEM)
SM = pl.BlockSpec(memory_space=pltpu.SMEM)


def square_index(n):
    return (
        lax.broadcasted_iota(jnp.int32, (n, n), 0),
        lax.broadcasted_iota(jnp.int32, (n, n), 1),
    )


def lay_out(scr, value):
    for j in range(scr.shape[0]):
        scr[j] = value[:, j * 128 : (j + 1) * 128].astype(F32)


def every(scr, start, count, stride):
    planes = [scr[j, pl.ds(start, count, stride=stride), :] for j in range(scr.shape[0])]
    return jnp.concatenate(planes, axis=1).astype(BF16)


def near(x):
    return pltpu.with_memory_space_constraint(x, pltpu.VMEM)


def place():
    rep = lax.axis_index("rep")
    return rep // SIDE, rep % SIDE, lax.axis_index("mp") % 2


def holder(first, second):
    y, x, other = place()
    ty = lax.rem(y + jnp.where(other == 0, second, first), SIDE)
    tx = lax.rem(x + jnp.where(other == 0, first, second), SIDE)
    return ty, tx


def swapping(n):
    row, col = square_index(n * n)
    return jnp.where(col == ((row & 15) << 4) + (row >> 4), 1.0, 0.0).astype(BF16)


def spread_rows(grads):
    rows, blocks, width = grads.shape
    n = 16

    def kernel(g_ref, *refs):
        outs, scr = refs[:SIDE], refs[SIDE]
        swap = swapping(n)
        for i in range(blocks // n):
            for h in range(rows // n):
                part = g_ref[n * h : n * (h + 1), n * i : n * (i + 1), :].reshape(n * n, width)
                part = mul(swap, part).astype(BF16)
                for k in range(n):
                    where = (n * i + k) // 2
                    scr[where, pl.ds((k % 2) * rows + n * h, n), :] = part[k * n : (k + 1) * n]
        for k in range(SIDE):
            for m in range(SIDE):
                ty, tx = holder(k, m)
                outs[k][m] = scr[SIDE * ty + tx]

    return pl.pallas_call(
        kernel,
        out_shape=(pltpu.VMEM((SIDE, 2 * rows, width), BF16),) * SIDE,
        in_specs=[VM],
        out_specs=(VM,) * SIDE,
        scratch_shapes=[pltpu.VMEM((blocks // 2, 2 * rows, width), BF16)],
        compiler_params=pltpu.CompilerParams(vmem_limit_bytes=12 << 20),
        name="spread_rows",
    )(grads)


def transpose_pieces(pieces):
    count = len(pieces)

    def kernel(*refs):
        for k in range(count):
            for m in range(count):
                refs[count + m][k] = refs[k][m]

    return pl.pallas_call(
        kernel,
        out_shape=(pltpu.VMEM(pieces[0].shape, BF16),) * count,
        in_specs=[VM] * count,
        out_specs=(VM,) * count,
        compiler_params=pltpu.CompilerParams(vmem_limit_bytes=12 << 20),
        name="transpose_pieces",
    )(*[near(piece) for piece in pieces])


def merge_rows(received):
    count, twice, width = received.shape
    rows = twice // 2
    blocks = 2 * count
    n = 16

    def kernel(r_ref, o_ref):
        swap = swapping(n)
        for i in range(blocks // n):
            for h in range(rows // n):
                part = jnp.concatenate(
                    [
                        r_ref[(n * i + k) // 2, pl.ds((k % 2) * rows + n * h, n), :]
                        for k in range(n)
                    ],
                    axis=0,
                )
                part = mul(swap, part).astype(BF16).reshape(n, n, width)
                o_ref[n * h : n * (h + 1), n * i : n * (i + 1), :] = part

    return pl.pallas_call(
        kernel,
        out_shape=jax.ShapeDtypeStruct((rows, blocks, width), BF16),
        in_specs=[VM],
        out_specs=VM,
        compiler_params=pltpu.CompilerParams(vmem_limit_bytes=12 << 20),
        name="merge_rows",
    )(near(received))


def step_along(value, shift, first):
    pairs = []
    groups = lax.axis_size("mp")
    for y in range(SIDE):
        for x in range(SIDE):
            for g in range(groups):
                along_x = (g % 2 == 0) == first
                ty, tx = (y, (x + shift) % SIDE) if along_x else ((y + shift) % SIDE, x)
                pairs.append(((SIDE * y + x) * groups + g, (SIDE * ty + tx) * groups + g))
    return lax.ppermute(value, ("rep", "mp"), pairs)


def lay_grams(scr, shifts, outs, tokens):
    half = scr.shape[3]
    width = 2 * half
    row, col = square_index(half)
    top_row = lax.broadcasted_iota(jnp.int32, (8, half), 0)
    for k, out in zip(shifts, outs):
        for m in range(SIDE):
            ty, tx = holder(k, m)
            last = jnp.zeros((8, half), F32)
            for q in range(2):
                v = every(scr.at[ty], 2 * tx + q, tokens, 2 * SIDE)
                gram = lax.dot_general(v, v, (((0,), (0,)), ((), ())), preferred_element_type=F32)
                low = gram[half:, half:]
                tri = jnp.where(row >= col, gram[:half, :half], low)
                out[m, q * width : q * width + half] = tri.astype(BF16)
                out[m, q * width + half : (q + 1) * width] = gram[:half, half:].astype(BF16)
                diagonal = jnp.sum(jnp.where(row == col, low, 0.0), axis=0, keepdims=True)
                last = jnp.where(top_row == q, diagonal, last)
            out[m, 2 * width :] = last.astype(BF16)


def first_grams(acts, shifts):
    tokens, _, width = acts.shape
    chunk = 2 * SIDE

    def kernel(a_hbm, *refs):
        outs, (scr, stage, sems) = refs[: len(shifts)], refs[len(shifts) :]
        copies = [
            pltpu.make_async_copy(a_hbm.at[:, pl.ds(chunk * i, chunk), :], stage.at[i], sems.at[i])
            for i in range(SIDE)
        ]
        for copy in copies:
            copy.start()
        for i in range(SIDE):
            copies[i].wait()
            lay_out(scr.at[i], stage[i].reshape(tokens * chunk, width))
        lay_grams(scr, shifts, outs, tokens)

    return pl.pallas_call(
        kernel,
        out_shape=(pltpu.VMEM((SIDE, 2 * width + 8, width // 2), BF16),) * len(shifts)
        + (pltpu.VMEM((SIDE, width // 128, tokens * chunk, 128), F32),),
        in_specs=[pl.BlockSpec(memory_space=pltpu.HBM)],
        out_specs=(VM,) * (len(shifts) + 1),
        scratch_shapes=[
            pltpu.VMEM((SIDE, tokens, chunk, width), BF16),
            pltpu.SemaphoreType.DMA((SIDE,)),
        ],
        compiler_params=pltpu.CompilerParams(vmem_limit_bytes=24 << 20),
        name="first_grams",
    )(pltpu.with_memory_space_constraint(acts, pltpu.HBM))


def other_grams(laid, shifts):
    half = laid.shape[3]
    tokens = laid.shape[2] // (2 * SIDE)

    def kernel(scr, *outs):
        lay_grams(scr, shifts, outs, tokens)

    return pl.pallas_call(
        kernel,
        out_shape=(pltpu.VMEM((SIDE, 4 * half + 8, half), BF16),) * len(shifts),
        in_specs=[VM],
        out_specs=(VM,) * len(shifts),
        compiler_params=pltpu.CompilerParams(vmem_limit_bytes=16 << 20),
        name="other_grams",
    )(near(laid))


def add_up(pieces):
    count, rows, half = pieces[0].shape

    def kernel(*refs):
        ins, outs = refs[: len(pieces)], refs[len(pieces) :]
        for m in range(count):
            total = ins[0][m].astype(F32)
            for ref in ins[1:]:
                total = total + ref[m].astype(F32)
            outs[m][...] = total.astype(outs[m].dtype)

    return pl.pallas_call(
        kernel,
        out_shape=(jax.ShapeDtypeStruct((rows, half), F32),)
        + (pltpu.VMEM((rows, half), BF16),) * (count - 1),
        in_specs=[VM] * len(pieces),
        out_specs=(VM,) * count,
        compiler_params=pltpu.CompilerParams(vmem_limit_bytes=12 << 20),
        name="add_up",
    )(*[near(piece) for piece in pieces])


def split(x):
    high = x.astype(BF16)
    return high, (x - high.astype(F32)).astype(BF16)


def mul(a, b):
    return lax.dot_general(a, b, (((1,), (0,)), ((), ())), preferred_element_type=F32)


def unpack(total, q, half):
    width = 2 * half
    row, col = square_index(half)
    tri = total[q * width : q * width + half]
    tri_t = tri.T
    cross = total[q * width + half : (q + 1) * width]
    diagonal = total[2 * width + q : 2 * width + q + 1]
    top = jnp.where(row >= col, tri, tri_t)
    low = jnp.where(row < col, tri, jnp.where(row > col, tri_t, diagonal))
    return jnp.concatenate(
        [jnp.concatenate([top, cross], axis=1), jnp.concatenate([cross.T, low], axis=1)], axis=0
    )


def refresh_blocks(pieces, damping, refresh, old_inverse, groups, tokens_all):
    slots, width, _ = old_inverse.shape
    half = width // 2

    def kernel(*refs):
        p_refs = refs[: len(pieces)]
        damp_ref, refresh_ref, old_ref, cov_ref, inv_ref, use_ref = refs[len(pieces) :]
        row, col = square_index(width)
        eye = jnp.where(row == col, 1.0, 0.0).astype(F32)
        total = p_refs[0][...].astype(F32)
        for ref in p_refs[1:]:
            total = total + ref[...].astype(F32)
        total = total * (1.0 / tokens_all)
        state = []
        for q in range(slots):
            cov = unpack(total, q, half)
            cov_ref[q] = cov
            matrix = cov + damp_ref[q] * eye
            bound = jnp.max(jnp.sum(jnp.abs(matrix), axis=0, keepdims=True), axis=1, keepdims=True)
            inv_bound = 1.0 / bound
            error = eye - matrix * inv_bound
            state.append((error, eye + error, inv_bound))
        for step in range(ITERS):
            following = []
            for error, series, inv_bound in state:
                e_high, e_low = split(error)
                if step == 0:
                    power = mul(e_high, e_high) + (mul(e_low, e_high) + mul(e_high, e_low))
                    following.append((power, series, inv_bound))
                    continue
                s_high, s_low = split(series)
                grown = mul(s_high, e_high) + (mul(s_low, e_high) + mul(s_high, e_low))
                power = error
                if step < ITERS - 1:
                    power = mul(e_high, e_high) + (mul(e_low, e_high) + mul(e_high, e_low))
                following.append((power, series + grown, inv_bound))
            state = following
        for q in range(slots):
            _, series, inv_bound = state[q]
            fresh = (series * inv_bound).astype(BF16)
            keep = (jnp.zeros((width, width), jnp.int32) + refresh_ref[q]) == groups
            inverse = jnp.where(keep, old_ref[q].astype(F32), fresh.astype(F32)).astype(BF16)
            inv_ref[q] = inverse
            use_ref[q] = inverse

    return pl.pallas_call(
        kernel,
        out_shape=(
            jax.ShapeDtypeStruct((slots, width, width), F32),
            jax.ShapeDtypeStruct((slots, width, width), BF16),
            pltpu.VMEM((slots, width, width), BF16),
        ),
        in_specs=[VM] * len(pieces) + [SM, SM, VM],
        out_specs=(VM,) * 3,
        compiler_params=pltpu.CompilerParams(vmem_limit_bytes=12 << 20),
        name="refresh_blocks",
    )(*[near(piece) for piece in pieces], damping, refresh, old_inverse)


def apply_inverse(pieces, inverse):
    _, twice, width = pieces[0].shape
    share = twice // 2

    def kernel(*refs):
        ins, (i_ref, o_ref) = refs[:SIDE], refs[SIDE:]
        for m in range(SIDE):
            for k in range(SIDE):
                ty, tx = holder(SIDE - k, SIDE - m)
                for q in range(2):
                    part = pl.ds(q * share, share)
                    o_ref[SIDE * ty + tx, part, :] = mul(ins[m][k, part, :], i_ref[q]).astype(BF16)

    return pl.pallas_call(
        kernel,
        out_shape=pltpu.VMEM((SIDE * SIDE, twice, width), BF16),
        in_specs=[VM] * (SIDE + 1),
        out_specs=VM,
        compiler_params=pltpu.CompilerParams(vmem_limit_bytes=12 << 20),
        name="apply_inverse",
    )(*[near(piece) for piece in pieces], near(inverse))


def ring(pieces, first, sign):
    moved = [pieces[0]]
    for k in range(1, SIDE):
        moved.append(step_along(pieces[k], (sign * k) % SIDE, first))
    return moved


def body(acts, refresh, damping, old_inverse, grads):
    replicas = lax.axis_size("rep")
    groups = lax.axis_size("mp")
    tokens_all = acts.shape[0] * replicas
    away, laid = first_grams(acts, (2,))
    ahead, behind, own = other_grams(laid, (1, 3, 0))
    pieces = ring((own, ahead, away, behind), True, 1)
    rows = spread_rows(grads)
    rows = ring(rows, True, 1)
    pieces = add_up(pieces)
    pieces = ring(pieces, False, 1)
    rows = transpose_pieces(rows)
    rows = ring(rows, False, 1)
    covariance, new_inverse, inverse = refresh_blocks(
        pieces, damping, refresh, old_inverse, groups, tokens_all
    )
    out = apply_inverse(rows, inverse)
    precond = merge_rows(lax.all_to_all(out, "rep", split_axis=0, concat_axis=0, tiled=True))
    return (covariance, new_inverse, precond)


def solution(mesh):
    return jax.shard_map(
        body,
        mesh=mesh,
        in_specs=(
            P("rep", "mp", None),
            P(("mp", "rep")),
            P(("mp", "rep")),
            P(("mp", "rep"), None, None),
            P("rep", "mp", None),
        ),
        out_specs=(
            P(("mp", "rep"), None, None),
            P(("mp", "rep"), None, None),
            P("rep", "mp", None),
        ),
        check_vma=False,
    )
```

```python
import jax
import jax.numpy as jnp
from jax import lax
from jax.experimental import pallas as pl
from jax.experimental.pallas import tpu as pltpu
from jax.sharding import PartitionSpec as P

ITERS = 5
SIDE = 4
FINE = 3
F32 = jnp.float32
BF16 = jnp.bfloat16
VM = pl.BlockSpec(memory_space=pltpu.VMEM)
SM = pl.BlockSpec(memory_space=pltpu.SMEM)


def square_index(n):
    return (
        lax.broadcasted_iota(jnp.int32, (n, n), 0),
        lax.broadcasted_iota(jnp.int32, (n, n), 1),
    )


def lay_out(scr, value):
    for j in range(scr.shape[0]):
        scr[j] = value[:, j * 128 : (j + 1) * 128].astype(F32)


def every(scr, start, count, stride):
    planes = [scr[j, pl.ds(start, count, stride=stride), :] for j in range(scr.shape[0])]
    return jnp.concatenate(planes, axis=1).astype(BF16)


def near(x):
    return pltpu.with_memory_space_constraint(x, pltpu.VMEM)


def place():
    rep = lax.axis_index("rep")
    return rep // SIDE, rep % SIDE, lax.axis_index("mp") % 2


def holder(first, second):
    y, x, other = place()
    ty = lax.rem(y + jnp.where(other == 0, second, first), SIDE)
    tx = lax.rem(x + jnp.where(other == 0, first, second), SIDE)
    return ty, tx


def swapping(n):
    row, col = square_index(n * n)
    return jnp.where(col == ((row & 15) << 4) + (row >> 4), 1.0, 0.0).astype(BF16)


def spread_rows(grads):
    rows, blocks, width = grads.shape
    n = 16

    def kernel(g_ref, *refs):
        outs, scr = refs[:SIDE], refs[SIDE]
        swap = swapping(n)
        for i in range(blocks // n):
            for h in range(rows // n):
                part = g_ref[n * h : n * (h + 1), n * i : n * (i + 1), :].reshape(n * n, width)
                part = mul(swap, part).astype(BF16)
                for k in range(n):
                    where = (n * i + k) // 2
                    scr[where, pl.ds((k % 2) * rows + n * h, n), :] = part[k * n : (k + 1) * n]
        for k in range(SIDE):
            for m in range(SIDE):
                ty, tx = holder(k, m)
                outs[k][m] = scr[SIDE * ty + tx]

    return pl.pallas_call(
        kernel,
        out_shape=(pltpu.VMEM((SIDE, 2 * rows, width), BF16),) * SIDE,
        in_specs=[VM],
        out_specs=(VM,) * SIDE,
        scratch_shapes=[pltpu.VMEM((blocks // 2, 2 * rows, width), BF16)],
        compiler_params=pltpu.CompilerParams(vmem_limit_bytes=12 << 20),
        name="spread_rows",
    )(grads)


def merge_rows(pieces):
    _, twice, width = pieces[0].shape
    rows = twice // 2
    blocks = 2 * SIDE * SIDE
    n = 16

    def kernel(*refs):
        ins, (o_ref, scr) = refs[:SIDE], refs[SIDE:]
        swap = swapping(n)
        for k in range(SIDE):
            for m in range(SIDE):
                ty, tx = holder(k, m)
                scr[SIDE * ty + tx] = ins[k][m]
        for i in range(blocks // n):
            for h in range(rows // n):
                part = jnp.concatenate(
                    [
                        scr[(n * i + k) // 2, pl.ds((k % 2) * rows + n * h, n), :]
                        for k in range(n)
                    ],
                    axis=0,
                )
                part = mul(swap, part).astype(BF16).reshape(n, n, width)
                o_ref[n * h : n * (h + 1), n * i : n * (i + 1), :] = part

    return pl.pallas_call(
        kernel,
        out_shape=jax.ShapeDtypeStruct((rows, blocks, width), BF16),
        in_specs=[VM] * SIDE,
        out_specs=VM,
        scratch_shapes=[pltpu.VMEM((blocks // 2, twice, width), BF16)],
        compiler_params=pltpu.CompilerParams(vmem_limit_bytes=12 << 20),
        name="merge_rows",
    )(*[near(piece) for piece in pieces])


def step_along(value, shift, first):
    pairs = []
    groups = lax.axis_size("mp")
    for y in range(SIDE):
        for x in range(SIDE):
            for g in range(groups):
                along_x = (g % 2 == 0) == first
                ty, tx = (y, (x + shift) % SIDE) if along_x else ((y + shift) % SIDE, x)
                pairs.append(((SIDE * y + x) * groups + g, (SIDE * ty + tx) * groups + g))
    return lax.ppermute(value, ("rep", "mp"), pairs)


def lay_grams(scr, shifts, outs, tokens):
    half = scr.shape[3]
    width = 2 * half
    row, col = square_index(half)
    top_row = lax.broadcasted_iota(jnp.int32, (8, half), 0)
    for k, out in zip(shifts, outs):
        for m in range(SIDE):
            ty, tx = holder(k, m)
            last = jnp.zeros((8, half), F32)
            for q in range(2):
                v = every(scr.at[ty], 2 * tx + q, tokens, 2 * SIDE)
                gram = lax.dot_general(v, v, (((0,), (0,)), ((), ())), preferred_element_type=F32)
                low = gram[half:, half:]
                tri = jnp.where(row >= col, gram[:half, :half], low)
                out[m, q * width : q * width + half] = tri.astype(BF16)
                out[m, q * width + half : (q + 1) * width] = gram[:half, half:].astype(BF16)
                diagonal = jnp.sum(jnp.where(row == col, low, 0.0), axis=0, keepdims=True)
                last = jnp.where(top_row == q, diagonal, last)
            out[m, 2 * width :] = last.astype(BF16)


def first_grams(acts, shifts):
    tokens, _, width = acts.shape
    chunk = 2 * SIDE

    def kernel(a_hbm, *refs):
        outs, (scr, stage, sems) = refs[: len(shifts)], refs[len(shifts) :]
        copies = [
            pltpu.make_async_copy(a_hbm.at[:, pl.ds(chunk * i, chunk), :], stage.at[i], sems.at[i])
            for i in range(SIDE)
        ]
        for copy in copies:
            copy.start()
        for i in range(SIDE):
            copies[i].wait()
            lay_out(scr.at[i], stage[i].reshape(tokens * chunk, width))
        lay_grams(scr, shifts, outs, tokens)

    return pl.pallas_call(
        kernel,
        out_shape=(pltpu.VMEM((SIDE, 2 * width + 8, width // 2), BF16),) * len(shifts)
        + (pltpu.VMEM((SIDE, width // 128, tokens * chunk, 128), F32),),
        in_specs=[pl.BlockSpec(memory_space=pltpu.HBM)],
        out_specs=(VM,) * (len(shifts) + 1),
        scratch_shapes=[
            pltpu.VMEM((SIDE, tokens, chunk, width), BF16),
            pltpu.SemaphoreType.DMA((SIDE,)),
        ],
        compiler_params=pltpu.CompilerParams(vmem_limit_bytes=24 << 20),
        name="first_grams",
    )(pltpu.with_memory_space_constraint(acts, pltpu.HBM))


def other_grams(laid, shifts):
    half = laid.shape[3]
    tokens = laid.shape[2] // (2 * SIDE)

    def kernel(scr, *outs):
        lay_grams(scr, shifts, outs, tokens)

    return pl.pallas_call(
        kernel,
        out_shape=(pltpu.VMEM((SIDE, 4 * half + 8, half), BF16),) * len(shifts),
        in_specs=[VM],
        out_specs=(VM,) * len(shifts),
        compiler_params=pltpu.CompilerParams(vmem_limit_bytes=16 << 20),
        name="other_grams",
    )(near(laid))


def add_up(pieces):
    count, rows, half = pieces[0].shape

    def kernel(*refs):
        ins, outs = refs[: len(pieces)], refs[len(pieces) :]
        for m in range(count):
            total = ins[0][m].astype(F32)
            for ref in ins[1:]:
                total = total + ref[m].astype(F32)
            outs[m][...] = total.astype(outs[m].dtype)

    return pl.pallas_call(
        kernel,
        out_shape=(pltpu.VMEM((rows, half), F32),)
        + (pltpu.VMEM((rows, half), BF16),) * (count - 1),
        in_specs=[VM] * len(pieces),
        out_specs=(VM,) * count,
        compiler_params=pltpu.CompilerParams(vmem_limit_bytes=12 << 20),
        name="add_up",
    )(*[near(piece) for piece in pieces])


def split(x):
    high = x.astype(BF16)
    return high, (x - high.astype(F32)).astype(BF16)


def mul(a, b):
    return lax.dot_general(a, b, (((1,), (0,)), ((), ())), preferred_element_type=F32)


def times(a, b, fine):
    if not fine:
        return mul(a[0], b[0])
    return mul(a[0], b[0]) + (mul(a[1], b[0]) + mul(a[0], b[1]))


def unpack(total, q, half):
    width = 2 * half
    row, col = square_index(half)
    tri = total[q * width : q * width + half]
    tri_t = tri.T
    cross = total[q * width + half : (q + 1) * width]
    diagonal = total[2 * width + q : 2 * width + q + 1]
    top = jnp.where(row >= col, tri, tri_t)
    low = jnp.where(row < col, tri, jnp.where(row > col, tri_t, diagonal))
    return jnp.concatenate(
        [jnp.concatenate([top, cross], axis=1), jnp.concatenate([cross.T, low], axis=1)], axis=0
    )


def refresh_blocks(pieces, damping, refresh, old_inverse, groups, tokens_all):
    slots, width, _ = old_inverse.shape
    half = width // 2

    def kernel(*refs):
        p_refs = refs[: len(pieces)]
        damp_ref, refresh_ref, old_ref, cov_ref, inv_ref = refs[len(pieces) :]
        row, col = square_index(width)
        eye = jnp.where(row == col, 1.0, 0.0).astype(F32)
        total = p_refs[0][...].astype(F32)
        for ref in p_refs[1:]:
            total = total + ref[...].astype(F32)
        total = total * (1.0 / tokens_all)
        state = []
        for q in range(slots):
            cov = unpack(total, q, half)
            cov_ref[q] = cov
            matrix = cov + damp_ref[q] * eye
            bound = jnp.max(jnp.sum(jnp.abs(matrix), axis=0, keepdims=True), axis=1, keepdims=True)
            inv_bound = 1.0 / bound
            error = eye - matrix * inv_bound
            state.append((error, eye + error, inv_bound))
        for step in range(ITERS):
            fine = step < FINE
            following = []
            for error, series, inv_bound in state:
                e_parts = split(error)
                power = error
                if step > 0:
                    series = series + times(split(series), e_parts, fine)
                if step < ITERS - 1:
                    power = times(e_parts, e_parts, fine)
                following.append((power, series, inv_bound))
            state = following
        for q in range(slots):
            _, series, inv_bound = state[q]
            fresh = (series * inv_bound).astype(BF16)
            keep = (jnp.zeros((width, width), jnp.int32) + refresh_ref[q]) == groups
            inverse = jnp.where(keep, old_ref[q].astype(F32), fresh.astype(F32)).astype(BF16)
            inv_ref[q] = inverse

    return pl.pallas_call(
        kernel,
        out_shape=(
            pltpu.VMEM((slots, width, width), F32),
            pltpu.VMEM((slots, width, width), BF16),
        ),
        in_specs=[VM] * len(pieces) + [SM, SM, VM],
        out_specs=(VM,) * 2,
        compiler_params=pltpu.CompilerParams(vmem_limit_bytes=12 << 20),
        name="refresh_blocks",
    )(*[near(piece) for piece in pieces], damping, refresh, old_inverse)


def apply_inverses(pieces, inverses):
    _, twice, width = pieces[0].shape
    share = twice // 2

    def kernel(*refs):
        ins, invs, outs = refs[:SIDE], refs[SIDE : 2 * SIDE], refs[2 * SIDE :]
        for m in range(SIDE):
            for q in range(2):
                part = pl.ds(q * share, share)
                flat = jnp.concatenate([ref[m, part, :] for ref in ins], axis=0)
                out = mul(flat, invs[m][q]).astype(BF16)
                for k in range(SIDE):
                    outs[k][m, part, :] = out[k * share : (k + 1) * share]

    return pl.pallas_call(
        kernel,
        out_shape=(pltpu.VMEM((SIDE, twice, width), BF16),) * SIDE,
        in_specs=[VM] * (2 * SIDE),
        out_specs=(VM,) * SIDE,
        compiler_params=pltpu.CompilerParams(vmem_limit_bytes=12 << 20),
        name="apply_inverses",
    )(*[near(piece) for piece in pieces], *[near(inverse) for inverse in inverses])


def ring(pieces, first, sign):
    moved = [pieces[0]]
    for k in range(1, SIDE):
        moved.append(step_along(pieces[k], (sign * k) % SIDE, first))
    return moved


def body(acts, refresh, damping, old_inverse, grads):
    replicas = lax.axis_size("rep")
    groups = lax.axis_size("mp")
    tokens_all = acts.shape[0] * replicas
    away, laid = first_grams(acts, (2,))
    ahead, behind, own = other_grams(laid, (1, 3, 0))
    pieces = ring((own, ahead, away, behind), True, 1)
    rows = spread_rows(grads)
    rows = ring(rows, True, 1)
    pieces = add_up(pieces)
    pieces = ring(pieces, False, 1)
    covariance, inverse = refresh_blocks(pieces, damping, refresh, old_inverse, groups, tokens_all)
    inverses = ring((inverse,) * SIDE, False, -1)
    out = apply_inverses(rows, inverses)
    out = ring(out, True, -1)
    precond = merge_rows(out)
    return (covariance, inverse, precond)


def solution(mesh):
    return jax.shard_map(
        body,
        mesh=mesh,
        in_specs=(
            P("rep", "mp", None),
            P(("mp", "rep")),
            P(("mp", "rep")),
            P(("mp", "rep"), None, None),
            P("rep", "mp", None),
        ),
        out_specs=(
            P(("mp", "rep"), None, None),
            P(("mp", "rep"), None, None),
            P("rep", "mp", None),
        ),
        check_vma=False,
    )
```
